32 devices in a mesh: section: 4 (over y, core), mp: 8 (over z, x).
Axes of the slice: x: 2, y: 2, z: 4, core: 2. Of those that a mesh axis runs over, the one named last changes fastest.
Arguments:
- arriving: bfloat16 [4, 768, 8192], P('section', None, 'mp'), may hold values from -6 to 6
- norm_gain: bfloat16 [4, 8192], P('section'), may hold values from 0.099609375 to 1.8984375
- w_query: bfloat16 [4, 2048, 8192], P('section', 'mp'), may hold values from -26 to 26
- w_key: bfloat16 [4, 1024, 8192], P('section', 'mp'), may hold values from -1 to 1
- w_value: bfloat16 [4, 1024, 8192], P('section', 'mp'), may hold values from -0.25 to 0.25
- w_out: bfloat16 [4, 2048, 8192], P('section', 'mp'), may hold values from -0.125 to 0.125
Outputs:
- attended: bfloat16 [4, 768, 8192], P('section', 'mp')
- stream_next: bfloat16 [4, 768, 8192], P('section', 'mp')
The draws below stay inside these ranges and needn't reach their ends.
All inputs are finite; a program needn't handle non-finite values.
Results may differ from the reference program's by a relative error of at most 0.017.
Values may be sent and summed in bfloat16 or wider, within the bound.
No kernel may reach another device: no remote copies, remote signals or barrier semaphores. Data moves between devices by JAX's collectives and lax.ppermute only.
A program may use at most 128 MiB of HBM per device.

```python
import math
import jax
import jax.numpy as jnp
from jax import lax

D = 8192
HD = 128
KV_HEADS = 8
HQ_DEV = 2
HEADS = 16
KVD = 1024
LENGTH = 768
SECTIONS = 4


def key_rows(key):
    fresh = jax.random.normal(jax.random.fold_in(key, 11), (SECTIONS, KVD, D), jnp.float32)
    return jnp.clip(fresh, -5.0, 5.0) / math.sqrt(D)


def draw_w_key(key, part):
    return key_rows(key).astype(jnp.bfloat16)


def draw_w_query(key, part):
    fresh = jax.random.normal(jax.random.fold_in(key, 23), (SECTIONS, HEADS * HD, D), jnp.float32)
    fresh = jnp.clip(fresh, -5.0, 5.0) / math.sqrt(D)
    return fresh.astype(jnp.bfloat16)


def shard_levels(own_key, shape, cuts, low, largest):
    level = 1.0
    for position, shards_of in cuts:
        draws = jax.random.uniform(jax.random.fold_in(jax.random.fold_in(own_key, 6), position), (shards_of,), jnp.float32, low / len(cuts), largest / len(cuts))
        level = level * jnp.repeat(jnp.exp(draws), shape[position] // shards_of).reshape((-1,) + (1,) * (len(shape) - 1 - position))
    return level


def gaussian(stream_key, shape, scale, most, split=(), held_as=jnp.bfloat16):
    drawn = scale * jax.random.normal(stream_key, shape, jnp.float32)
    if split:
        drawn = drawn * shard_levels(stream_key, shape, split, -0.22, 0.18)
    return jnp.clip(drawn, -most, most).astype(held_as)


def setup_inputs(seed: int = 0) -> dict:
    splits = jax.random.split(jax.random.key(seed), 7)
    return {
        "arriving": gaussian(splits[0], (SECTIONS, LENGTH, D), 1.0, 6.0, ((0, 4), (2, 8))),
        "norm_gain": jnp.clip(1.0 + 0.18 * jax.random.normal(splits[1], (SECTIONS, D), jnp.float32), 0.099609375, 1.8984375).astype(jnp.bfloat16),
        "w_query": draw_w_query(jax.random.fold_in(splits[6], 71), 0),
        "w_key": draw_w_key(jax.random.fold_in(splits[6], 71), 0),
        "w_value": gaussian(splits[4], (SECTIONS, KVD, D), (D // 16) ** -0.5, 0.25, ((0, 4), (1, 8))),
        "w_out": gaussian(splits[5], (SECTIONS, HEADS * HD, D), (HEADS * HD) ** -0.5, 0.125, ((0, 4), (1, 8))),
    }


rope_base = 500000.0
norm_eps = 1e-05

def rotate(channel_major, first_channel):
    channels = channel_major.shape[0]
    length = channel_major.shape[1]
    within = (jnp.arange(channels, dtype=jnp.int32) + first_channel) % HD
    pair_index = (within // 2).astype(channel_major.dtype)
    frequency = jnp.exp(pair_index * (-2.0 * math.log(rope_base) / HD))
    positions = jnp.arange(length, dtype=jnp.int32).astype(channel_major.dtype)
    angles = frequency[0::2, None] * positions[None, :]
    cos_table = jnp.cos(angles)
    sine_table = jnp.sin(angles)
    paired = channel_major.reshape(channels // 2, 2, length)
    even_part = paired[:, 0]
    odd_part = paired[:, 1]
    rotated = jnp.stack([even_part * cos_table - odd_part * sine_table, even_part * sine_table + odd_part * cos_table], axis=1)
    return rotated.reshape(channels, length)

def head_order(pair_major):
    length = pair_major.shape[1]
    grouped = pair_major.reshape(HD // 2, KV_HEADS, 2, length)
    return jnp.transpose(grouped, (1, 0, 2, 3)).reshape(KV_HEADS * HD, length)

def normalize(hidden_in, gain_row):
    as_float = hidden_in.astype(jnp.float32)
    mean_square = lax.optimization_barrier(jnp.mean(as_float * as_float, axis=1, keepdims=True))
    normed = (as_float * lax.rsqrt(mean_square + norm_eps) * gain_row.astype(jnp.float32)).astype(jnp.bfloat16)
    return (as_float, normed)

def reference(arriving, norm_gain, w_query, w_key, w_value, w_out):
    group_size = HEADS // KV_HEADS
    width = HQ_DEV * HD
    score_scale = 1.0 / math.sqrt(HD)
    attended_all = []
    stream_all = []
    for section in range(SECTIONS):
        as_float, normed = normalize(arriving[(section - 1) % SECTIONS], norm_gain[section])
        length = normed.shape[0]
        queries = rotate(jnp.dot(w_query[section], normed.T, preferred_element_type=jnp.float32), 0).astype(jnp.bfloat16)
        key_all = rotate(head_order(jnp.dot(w_key[section], normed.T, preferred_element_type=jnp.float32)), 0).astype(jnp.bfloat16)
        value_all = head_order(jnp.dot(w_value[section], normed.T, preferred_element_type=jnp.float32)).astype(jnp.bfloat16)
        query_heads = queries.reshape(HEADS, HD, length).astype(jnp.float32)
        key_heads = jnp.repeat(key_all.reshape(KV_HEADS, HD, length), group_size, axis=0).astype(jnp.float32)
        value_heads = jnp.repeat(value_all.reshape(KV_HEADS, HD, length), group_size, axis=0).astype(jnp.float32)
        scores = jnp.einsum('hdi,hdj->hij', query_heads, key_heads) * score_scale
        token_index = jnp.arange(length, dtype=jnp.int32)
        causal = token_index[:, None] >= token_index[None, :]
        scores = jnp.where(causal[None], scores, -1e+30)
        row_max = lax.optimization_barrier(jnp.max(scores, axis=-1, keepdims=True))
        exponent = jnp.exp(scores - row_max)
        row_total = lax.optimization_barrier(jnp.sum(exponent, axis=-1, keepdims=True))
        weights = (exponent / row_total).astype(jnp.bfloat16)
        context = jnp.einsum('hij,hdj->ihd', weights.astype(jnp.float32), value_heads).astype(jnp.bfloat16)
        context = context.reshape(length, HEADS * HD)
        summed = jnp.zeros((length, D), jnp.float32)
        for shard in range(HEADS // HQ_DEV):
            partial_term = jnp.dot(context[:, shard * width:(shard + 1) * width], w_out[section][shard * width:(shard + 1) * width], preferred_element_type=jnp.float32)
            summed = summed + lax.optimization_barrier(partial_term.astype(jnp.bfloat16)).astype(jnp.float32)
        attended_all.append(summed.astype(jnp.bfloat16))
        stream_all.append((as_float + summed).astype(jnp.bfloat16))
    return (jnp.stack(attended_all), jnp.stack(stream_all))
```

```python
import math

import jax
import jax.numpy as jnp
import numpy as np
from jax import lax
from jax.sharding import PartitionSpec as P


HD = 128
KV_HEADS = 8


rope_base = 500000.0
norm_eps = 1e-05


def ring_index(position, count):
    half = count // 2
    if isinstance(position, int):
        return 2 * position if position < half else 2 * (count - 1 - position) + 1
    return jnp.where(position < half, 2 * position, 2 * (count - 1 - position) + 1)


def rotate(parts, pair_ids):
    length = parts.shape[-1]
    frequency = jnp.exp(pair_ids.astype(jnp.float32) * (-2.0 * math.log(rope_base) / HD))
    positions = jnp.arange(length, dtype=jnp.int32).astype(jnp.float32)
    angles = frequency[..., None] * positions
    cos_table = jnp.cos(angles)
    sine_table = jnp.sin(angles)
    even_part = parts[:, 0]
    odd_part = parts[:, 1]
    return jnp.stack(
        [
            even_part * cos_table - odd_part * sine_table,
            even_part * sine_table + odd_part * cos_table,
        ],
        axis=1,
    )


def layer(arriving, norm_gain, w_query, w_key, w_value, w_out):
    local_block = arriving[0]
    gain_row = norm_gain[0].astype(jnp.float32)
    out_weights = w_out[0]
    mp_count = lax.axis_size("mp")
    member = lax.axis_index("mp")
    length, width = local_block.shape
    features = width * mp_count
    half = width // 2
    row_count = length // mp_count
    place = jnp.where(member % 2 == 0, member // 2, mp_count - 1 - member // 2)
    order = [ring_index(i, mp_count) for i in range(mp_count)]
    ahead = [(order[i], order[(i + 1) % mp_count]) for i in range(mp_count)]
    behind = [(b, a) for a, b in ahead]
    sections = lax.axis_size("section")

    def next_section(routes):
        return [
            (section * mp_count + a, (section + 1) % sections * mp_count + b)
            for section in range(sections)
            for a, b in routes
        ]

    q_width = w_query.shape[1]
    k_width = w_key.shape[1]
    local_heads = q_width // HD
    pair_count = k_width // (2 * KV_HEADS)
    groups = HD // 2 // pair_count
    q_rows = np.arange(q_width).reshape(local_heads * groups, pair_count, 2).transpose(0, 2, 1)
    kv_rows = np.arange(k_width).reshape(pair_count, KV_HEADS, 2)
    source_rows = np.concatenate(
        [
            q_rows.reshape(-1),
            q_width + kv_rows.transpose(1, 2, 0).reshape(-1),
            q_width + k_width + kv_rows.transpose(1, 0, 2).reshape(-1),
        ]
    )
    stacked = jnp.concatenate([w_query[0], w_key[0], w_value[0]], axis=0)
    selector = jnp.asarray(source_rows, jnp.int32)[:, None] == jnp.arange(stacked.shape[0])
    weights_all = lax.optimization_barrier(
        jnp.dot(
            selector.astype(jnp.bfloat16), stacked, preferred_element_type=jnp.float32
        ).astype(jnp.bfloat16)
    )

    both = ("section", "mp")
    forward = lax.ppermute(local_block[:, :half], both, next_section(ahead))
    backward = lax.ppermute(local_block[:, half:], both, next_section(behind))
    own = lax.ppermute(local_block, both, next_section([(i, i) for i in range(mp_count)]))

    projected = jnp.zeros((weights_all.shape[0], length), jnp.float32)
    square_sum = jnp.zeros((length,), jnp.float32)
    residual = jnp.zeros((row_count, features), jnp.bfloat16)

    def take(state, block, source, start):
        projected, square_sum, residual = state
        size = block.shape[1]
        offset = source * width + start
        gain = lax.dynamic_slice_in_dim(gain_row, offset, size, 0)
        block_float = block.astype(jnp.float32)
        columns = lax.dynamic_slice_in_dim(weights_all, offset, size, 1)
        projected = projected + lax.dot_general(
            columns,
            (block_float * gain).astype(jnp.bfloat16),
            (((1,), (1,)), ((), ())),
            preferred_element_type=jnp.float32,
        )
        square_sum = square_sum + jnp.sum(block_float * block_float, axis=1)
        rows = lax.dynamic_slice_in_dim(block, member * row_count, row_count, 0)
        residual = lax.dynamic_update_slice(residual, rows, (jnp.int32(0), offset))
        return lax.optimization_barrier(projected), square_sum, residual

    state = (projected, square_sum, residual)
    for step in range(1, mp_count):
        source_f = ring_index((place - step) % mp_count, mp_count)
        source_b = ring_index((place + step) % mp_count, mp_count)
        if step + 1 < mp_count:
            next_f = lax.ppermute(forward, "mp", ahead)
            next_b = lax.ppermute(backward, "mp", behind)
        state = take(state, forward, source_f, 0)
        state = take(state, backward, source_b, half)
        if step == 3:
            state = take(state, own, member, 0)
        forward, backward = next_f, next_b
    projected, square_sum, residual = state
    projected = projected * lax.rsqrt(square_sum / features + norm_eps)

    key_pairs = member * pair_count + jnp.arange(pair_count, dtype=jnp.int32)
    key_part = projected[q_width : q_width + k_width].reshape(KV_HEADS, 2, pair_count, length)
    key_part = rotate(key_part, key_pairs[None]).astype(jnp.bfloat16)
    key_part = key_part.reshape(KV_HEADS, 1, 2 * pair_count, length)
    value_part = projected[q_width + k_width :].astype(jnp.bfloat16)
    value_part = value_part.reshape(KV_HEADS, 1, 2 * pair_count, length)
    outgoing = jnp.concatenate([key_part, value_part], axis=1)
    outgoing = jnp.repeat(outgoing, mp_count // KV_HEADS, axis=0)
    incoming = lax.all_to_all(outgoing, "mp", 0, 0, tiled=True)
    key_head = incoming[:, 0].reshape(HD, length)
    value_head = incoming[:, 1].reshape(HD, length)

    query_pairs = jnp.arange(local_heads * groups, dtype=jnp.int32)[:, None] % groups
    query_pairs = query_pairs * pair_count + jnp.arange(pair_count, dtype=jnp.int32)[None]
    query_part = projected[:q_width].reshape(local_heads * groups, 2, pair_count, length)
    query_heads = rotate(query_part, query_pairs).astype(jnp.bfloat16)
    query_heads = query_heads.reshape(local_heads, HD, length)

    score_scale = 1.0 / math.sqrt(HD)
    scores = (
        jnp.einsum("hdi,dj->hij", query_heads, key_head, preferred_element_type=jnp.float32)
        * score_scale
    )
    token_index = jnp.arange(length, dtype=jnp.int32)
    causal = token_index[:, None] >= token_index[None, :]
    scores = jnp.where(causal[None], scores, -1e30)
    row_max = jnp.max(scores, axis=-1, keepdims=True)
    exponent = jnp.exp(scores - row_max)
    row_total = jnp.sum(exponent, axis=-1, keepdims=True)
    weights = (exponent / row_total).astype(jnp.bfloat16)
    context = jnp.einsum(
        "hij,dj->ihd", weights, value_head, preferred_element_type=jnp.float32
    ).astype(jnp.bfloat16)
    context = context.reshape(length, q_width)

    def term(dest, start):
        rows = lax.dynamic_slice_in_dim(context, dest * row_count, row_count, 0)
        columns = out_weights[:, start : start + features // 2]
        product = jnp.dot(rows, columns, preferred_element_type=jnp.float32)
        return lax.optimization_barrier(product.astype(jnp.bfloat16)).astype(jnp.float32)

    sum_f = sum_b = None
    for step in range(mp_count):
        dest_f = ring_index((place - 1 - step) % mp_count, mp_count)
        dest_b = ring_index((place + 1 + step) % mp_count, mp_count)
        term_f = term(dest_f, 0)
        term_b = term(dest_b, features // 2)
        sum_f = term_f if sum_f is None else term_f + sum_f.astype(jnp.float32)
        sum_b = term_b if sum_b is None else term_b + sum_b.astype(jnp.float32)
        if step + 1 < mp_count:
            sum_f = lax.ppermute(sum_f.astype(jnp.bfloat16), "mp", ahead)
            sum_b = lax.ppermute(sum_b.astype(jnp.bfloat16), "mp", behind)
    summed = jnp.concatenate([sum_f, sum_b], axis=1)
    attended = summed.astype(jnp.bfloat16)[None]
    stream_next = (residual.astype(jnp.float32) + summed).astype(jnp.bfloat16)[None]
    return (attended, stream_next)


def solution(mesh):
    return jax.shard_map(
        layer,
        mesh=mesh,
        in_specs=(
            P("section", None, "mp"),
            P("section", None),
            P("section", "mp", None),
            P("section", "mp", None),
            P("section", "mp", None),
            P("section", "mp", None),
        ),
        out_specs=(P("section", "mp", None), P("section", "mp", None)),
        check_vma=False,
    )
```
